32 devices in a mesh: tm: 2 (over x), member: 4 (over y, core), state: 4 (over z).
Axes of the slice: x: 2, y: 2, z: 4, core: 2. Of those that a mesh axis runs over, the one named last changes fastest.
Arguments:
- members: bfloat16 [4, 8, 16, 192, 1536], P('tm', 'member', None, 'state'), may hold values from -6 to 6
- slot_grad: float32 [4, 16, 192, 1536], P('tm', None, 'state'), may hold values from -6 to 6
- diffusivity: float32 [192, 1536], P('state'), may hold values from 0.03 to 0.24
- vertical: float32 [16, 16], replicated, may hold values from -0.3 to 2.1, as said below
Outputs:
- control_gradient: float32 [16, 8, 192, 1536], P('tm', 'member', 'state')
The draws below stay inside these ranges and needn't reach their ends.
Inputs may be any that keep to these rules, and one draw needn't show every extreme that they name: `vertical`: the diagonal entries lie between 0.5 and 2.1.
All inputs are finite; a program needn't handle non-finite values.
Results may differ from the reference program's by a relative error of at most 0.0003.
Values sent between devices are 32-bit elements; how exact they have to be, the bound alone decides.
A program may use at most 128 MiB of HBM per device.

```python
import math
import jax
import jax.numpy as jnp
from jax import lax

LON = 1536
LEVELS = 16
NSTEP = 4
LAT = 192
MEMBERS = 8
SLOTS = 4


def draw_vertical(key, part):
    first_key, second_key = jax.random.split(jax.random.fold_in(key, 17))
    offdiag = jnp.clip(jax.random.normal(first_key, (LEVELS, LEVELS), jnp.float32), -3.0, 3.0) / 3.0
    diagonal = jnp.exp(jax.random.uniform(second_key, (LEVELS,), jnp.float32, -0.69, 0.69))
    identity = jnp.eye(LEVELS, dtype=jnp.float32)
    return 0.27 * offdiag * (1.0 - identity) + identity * diagonal[None, :]


def levels(stream_key, shape, pieces, smallest, top_value):
    level, own = 1.0, jax.random.fold_in(stream_key, 6)
    for axis_at, parts in pieces:
        heights = jnp.exp(jax.random.uniform(jax.random.fold_in(own, axis_at), (parts,), jnp.float32, smallest / len(pieces), top_value / len(pieces)))
        level = level * jnp.repeat(heights, shape[axis_at] // parts).reshape([-1 if axis == axis_at else 1 for axis in range(len(shape))])
    return level


def noise(stream_key, shape, width, limit, cuts=(), kind=jnp.bfloat16):
    gain = levels(stream_key, shape, cuts, -0.22, 0.18) if cuts else 1.0
    result = jax.random.normal(stream_key, shape, jnp.float32) * width * gain
    return jnp.minimum(jnp.maximum(result, -limit), limit).astype(kind)


def setup_inputs(seed: int = 0) -> dict:
    key_of = jax.random.split(jax.random.key(seed), 5)
    members = noise(key_of[0], (SLOTS, MEMBERS, LEVELS, LAT, LON), 1.0, 6.0, ((0, 2), (1, 4), (3, 4)))
    slot_grad = noise(key_of[1], (SLOTS, LEVELS, LAT, LON), 1.0, 6.0, ((0, 2), (2, 4)), jnp.float32)
    diffusivity = jnp.clip(jnp.exp(math.log(0.24) - 2.0794415 * jax.random.uniform(key_of[2], (LAT, LON), jnp.float32) ** levels(key_of[2], (LAT, LON), ((0, 4),), -0.2, 0.2)), 0.03, 0.24)
    vertical = draw_vertical(jax.random.fold_in(key_of[4], 71), 0)
    return dict(members=members, slot_grad=slot_grad, diffusivity=diffusivity, vertical=vertical)


def stencil_update(centre, spread):
    middle = spread[..., 1:-1, :]
    return centre + spread[..., 2:, :] + spread[..., :-2, :] + jnp.roll(middle, 1, -1) + jnp.roll(middle, -1, -1) - 4.0 * middle


def reference(members, slot_grad, diffusivity, vertical):
    ensemble = members.shape[1]
    spread_scale = float(ensemble - 1) ** -0.5
    centre = jnp.sum(members, axis=1, dtype=jnp.float32) / ensemble

    def member_product(which):
        single = lax.dynamic_index_in_dim(members, which, 1, keepdims=False).astype(jnp.float32)
        perturbed = (single - centre) * spread_scale
        return jnp.sum(perturbed * slot_grad, axis=0)

    partial_value = lax.map(member_product, jnp.arange(ensemble, dtype=jnp.int32))
    field = jnp.einsum("ml,kmab->lkab", vertical, partial_value, precision=lax.Precision.HIGHEST)
    for step_index in range(NSTEP):
        spread = jnp.pad(diffusivity * field, ((0, 0), (0, 0), (1, 1), (0, 0)))
        field = stencil_update(field, spread)
    return field
```

```python
import functools

import jax
import jax.numpy as jnp
from jax import lax
from jax.experimental import pallas as pl
from jax.experimental.pallas import tpu as pltpu
from jax.sharding import PartitionSpec as P

NSTEP = 4
HALO = 8
CHUNK = 16
VMEM_BYTES = 64 * 1000 * 1000


def kernel(
    tm_size, member_size, state_size, scale,
    members_ref, grad_ref, diff_ref, vertical_ref, out_ref,
    mem_v, grad_v, part, send, recv, field, local_sum, total, rs_buf, edges,
    diff_v, fbuf, va, vb,
    in_sem, diff_sem, xs_sem, xr_sem, rss_sem, rsr_sem, ags_sem, agr_sem,
    hs_sem, hr_sem, ds_sem, dr_sem, out_sem,
):
    slots, local, levels, rows, cols = mem_v.shape
    out_levels = field.shape[0]
    ensemble = local * member_size
    width = cols // member_size
    tm = lax.axis_index("tm")
    mine = lax.axis_index("member")
    state = lax.axis_index("state")
    has_up, has_down = state > 0, state < state_size - 1
    chunks = rows // CHUNK

    def in_copies(c):
        at = pl.ds(c * CHUNK, CHUNK)
        return (
            pltpu.make_async_copy(
                members_ref.at[:, :, :, at, :], mem_v.at[:, :, :, at, :], in_sem.at[0, c]
            ),
            pltpu.make_async_copy(grad_ref.at[:, :, at, :], grad_v.at[:, :, at, :], in_sem.at[1, c]),
        )

    for c in range(chunks):
        for copy in in_copies(c):
            copy.start()
    diff_in = pltpu.make_async_copy(diff_ref, diff_v.at[pl.ds(HALO, rows), :], diff_sem)
    diff_in.start()

    barrier = pltpu.get_barrier_semaphore()
    for d in range(1, tm_size):
        pl.semaphore_signal(barrier, inc=1, device_id={"tm": lax.rem(tm + d, tm_size)})
    for d in range(1, member_size):
        pl.semaphore_signal(barrier, inc=1, device_id={"member": lax.rem(mine + d, member_size)})

    @pl.when(has_up)
    def _():
        pl.semaphore_signal(barrier, inc=1, device_id={"state": state - 1})

    @pl.when(has_down)
    def _():
        pl.semaphore_signal(barrier, inc=1, device_id={"state": state + 1})

    sides = has_up.astype(jnp.int32) + has_down.astype(jnp.int32)
    pl.semaphore_wait(barrier, tm_size + member_size - 2 + sides)

    def x_copy(d, lev, at):
        return pltpu.make_async_remote_copy(
            src_ref=send.at[d - 1, lev, :, at, :],
            dst_ref=recv.at[d - 1, lev, :, at, :],
            send_sem=xs_sem.at[d - 1, lev],
            recv_sem=xr_sem.at[d - 1, lev],
            device_id={"tm": lax.rem(tm + d, tm_size)},
        )

    def mix(source_level, dst, tile0, tiles):
        def one(i, carry):
            m = lax.rem(i, local)
            at = pl.ds(pl.multiple_of((tile0 + i // local) * 8, 8), 8)
            acc = vertical_ref[0, source_level] * part[0, m, at, :]
            for j in range(1, levels):
                acc = acc + vertical_ref[j, source_level] * part[j, m, at, :]
            dst[m, at, :] = acc
            return carry

        lax.fori_loop(0, tiles * local, one, 0)

    def send_level(d, lev):
        return lax.rem(tm + d, tm_size) * out_levels + lev

    for c in range(chunks):
        at = pl.ds(c * CHUNK, CHUNK)
        for copy in in_copies(c):
            copy.wait()

        def slot_sum(j, carry):
            for m in range(local):
                acc = mem_v[0, m, j, at, :].astype(jnp.float32) * grad_v[0, j, at, :]
                for s in range(1, slots):
                    acc = acc + mem_v[s, m, j, at, :].astype(jnp.float32) * grad_v[s, j, at, :]
                part[j, m, at, :] = acc
            return carry

        lax.fori_loop(0, levels, slot_sum, 0)
        for d in range(1, tm_size):
            mix(send_level(d, 0), send.at[d - 1, 0], c * (CHUNK // 8), CHUNK // 8)
            x_copy(d, 0, at).start()

    full = pl.ds(0, rows)

    def send_rest(lev, carry):
        for d in range(1, tm_size):
            mix(send_level(d, lev), send.at[d - 1, lev], 0, rows // 8)
            x_copy(d, lev, full).start()
        return carry

    lax.fori_loop(1, out_levels, send_rest, 0)

    diff_in.wait()

    def neighbour_copy(up, src, dst, send_sem, recv_sem):
        return pltpu.make_async_remote_copy(
            src_ref=src,
            dst_ref=dst,
            send_sem=send_sem,
            recv_sem=recv_sem,
            device_id={"state": state - 1 if up else state + 1},
        )

    def diff_copy(up):
        src = HALO if up else rows
        dst = rows + HALO if up else 0
        k = 1 if up else 0
        return neighbour_copy(
            up, diff_v.at[pl.ds(src, HALO), :], diff_v.at[pl.ds(dst, HALO), :], ds_sem.at[k], dr_sem.at[k]
        )

    def edge_copy(up, lev):
        src = 0 if up else rows - HALO
        k = 1 if up else 0
        return neighbour_copy(
            up, field.at[lev, :, pl.ds(src, HALO), :], edges.at[lev, k], hs_sem.at[k, lev], hr_sem.at[k, lev]
        )

    @pl.when(has_up)
    def _():
        diff_copy(True).start()

    @pl.when(has_down)
    def _():
        diff_copy(False).start()

    def clear_edges(k):
        diff_v[pl.ds(k * (rows + HALO), HALO), :] = jnp.zeros((HALO, cols), jnp.float32)

        def one(lev, carry):
            edges[lev, k] = jnp.zeros(edges.shape[2:], jnp.float32)
            return carry

        lax.fori_loop(0, out_levels, one, 0)

    @pl.when(jnp.logical_not(has_up))
    def _():
        clear_edges(0)

    @pl.when(jnp.logical_not(has_down))
    def _():
        clear_edges(1)

    for v in (va, vb):
        for m in range(local):
            v[m, pl.ds(0, 8), :] = jnp.zeros((8, cols), jnp.float32)
            v[m, pl.ds(rows + 2 * HALO + 8, 8), :] = jnp.zeros((8, cols), jnp.float32)

    def own(lev, carry):
        mix(tm * out_levels + lev, field.at[lev], 0, rows // 8)
        return carry

    lax.fori_loop(0, out_levels, own, 0)

    @pl.when(has_up)
    def _():
        diff_copy(True).wait_send()
        diff_copy(False).wait_recv()

    @pl.when(has_down)
    def _():
        diff_copy(False).wait_send()
        diff_copy(True).wait_recv()

    def lane_slice(owner):
        return pl.ds(pl.multiple_of(owner * width, 128), width)

    def rs_copy(d, lev):
        peer = lax.rem(mine + d, member_size)
        return pltpu.make_async_remote_copy(
            src_ref=local_sum.at[lev, :, lane_slice(peer)],
            dst_ref=rs_buf.at[lev, d - 1],
            send_sem=rss_sem.at[d - 1, lev],
            recv_sem=rsr_sem.at[d - 1, lev],
            device_id={"member": peer},
        )

    def ag_copy(d, lev, owner):
        return pltpu.make_async_remote_copy(
            src_ref=total.at[lev, :, lane_slice(owner)],
            dst_ref=total.at[lev, :, lane_slice(owner)],
            send_sem=ags_sem.at[d - 1, lev],
            recv_sem=agr_sem.at[d - 1, lev],
            device_id={"member": lax.rem(mine + d, member_size)},
        )

    def arrive(lev):
        for d in range(1, tm_size):
            x_copy(d, lev, full).wait_recv()

        def one(i, carry):
            at = pl.ds(pl.multiple_of(i * 8, 8), 8)
            acc = None
            for m in range(local):
                value = field[lev, m, at, :]
                for d in range(1, tm_size):
                    value = value + recv[d - 1, lev, m, at, :]
                field[lev, m, at, :] = value
                acc = value if acc is None else acc + value
            local_sum[lev, at, :] = acc
            return carry

        lax.fori_loop(0, rows // 8, one, 0)
        for d in range(1, member_size):
            rs_copy(d, lev).start()

    def reduce(lev):
        for d in range(1, member_size):
            rs_copy(d, lev).wait_recv()
        at = lane_slice(mine)
        acc = local_sum[lev, :, at]
        for d in range(1, member_size):
            acc = acc + rs_buf[lev, d - 1]
        total[lev, :, at] = acc * (1.0 / ensemble)
        for d in range(1, member_size):
            ag_copy(d, lev, mine).start()

    def centre(lev):
        for d in range(1, member_size):
            ag_copy(d, lev, lax.rem(mine + member_size - d, member_size)).wait_recv()

        def one(i, carry):
            at = pl.ds(pl.multiple_of(i * 8, 8), 8)
            mean = total[lev, at, :]
            for m in range(local):
                field[lev, m, at, :] = (field[lev, m, at, :] - mean) * scale
            return carry

        lax.fori_loop(0, rows // 8, one, 0)

        @pl.when(has_up)
        def _():
            edge_copy(True, lev).start()

        @pl.when(has_down)
        def _():
            edge_copy(False, lev).start()

    tiles = (rows + 2 * HALO) // 8

    def filter_level(lev):
        @pl.when(has_up)
        def _():
            edge_copy(True, lev).wait_send()
            edge_copy(False, lev).wait_recv()

        @pl.when(has_down)
        def _():
            edge_copy(False, lev).wait_send()
            edge_copy(True, lev).wait_recv()

        def one(m, carry):
            for i in range(tiles):
                if i == 0:
                    value = edges[lev, 0, m]
                elif i == tiles - 1:
                    value = edges[lev, 1, m]
                else:
                    value = field[lev, m, pl.ds(8 * (i - 1), 8), :]
                fbuf[m, pl.ds(8 * i, 8), :] = value
                va[m, pl.ds(8 * i + 8, 8), :] = value * diff_v[pl.ds(8 * i, 8), :]
            now, later = va, vb
            for step in range(NSTEP):
                last = step == NSTEP - 1
                for i in range(1 if last else 0, tiles - 1 if last else tiles):
                    mid = now[m, pl.ds(8 * i + 8, 8), :]
                    value = (
                        fbuf[m, pl.ds(8 * i, 8), :]
                        + now[m, pl.ds(8 * i + 9, 8), :]
                        + now[m, pl.ds(8 * i + 7, 8), :]
                        + pltpu.roll(mid, 1, 1)
                        + pltpu.roll(mid, cols - 1, 1)
                        - 4.0 * mid
                    )
                    if last:
                        field[lev, m, pl.ds(8 * (i - 1), 8), :] = value
                    else:
                        fbuf[m, pl.ds(8 * i, 8), :] = value
                        later[m, pl.ds(8 * i + 8, 8), :] = value * diff_v[pl.ds(8 * i, 8), :]
                now, later = later, now
            return carry

        lax.fori_loop(0, local, one, 0)
        out_copy(lev).start()

    def out_copy(lev):
        return pltpu.make_async_copy(field.at[lev], out_ref.at[lev], out_sem.at[lev])

    arrive(0)
    reduce(0)

    def step(lev, carry):
        arrive(lev)
        centre(lev - 1)
        reduce(lev)
        filter_level(lev - 1)
        return carry

    lax.fori_loop(1, out_levels, step, 0)
    centre(out_levels - 1)
    filter_level(out_levels - 1)

    def finish(lev, carry):
        for d in range(1, tm_size):
            x_copy(d, lev, full).wait_send()
        for d in range(1, member_size):
            rs_copy(d, lev).wait_send()
            ag_copy(d, lev, mine).wait_send()
        out_copy(lev).wait()
        return carry

    lax.fori_loop(0, out_levels, finish, 0)


def solution(mesh):
    tm_size, member_size, state_size = (mesh.shape[a] for a in ("tm", "member", "state"))

    def body(members, slot_grad, diffusivity, vertical):
        slots, local, levels, rows, cols = members.shape
        out_levels = levels // tm_size
        width = cols // member_size
        f32 = jnp.float32
        dma = pltpu.SemaphoreType.DMA
        chunks = rows // CHUNK
        scale = float(local * member_size - 1) ** -0.5
        block = (out_levels, local, rows, cols)
        padded = (local, rows + 2 * HALO + 16, cols)
        scratch = [
            pltpu.VMEM(members.shape, members.dtype),
            pltpu.VMEM(slot_grad.shape, f32),
            pltpu.VMEM((levels, local, rows, cols), f32),
            pltpu.VMEM((tm_size - 1,) + block, f32),
            pltpu.VMEM((tm_size - 1,) + block, f32),
            pltpu.VMEM(block, f32),
            pltpu.VMEM((out_levels, rows, cols), f32),
            pltpu.VMEM((out_levels, rows, cols), f32),
            pltpu.VMEM((out_levels, member_size - 1, rows, width), f32),
            pltpu.VMEM((out_levels, 2, local, HALO, cols), f32),
            pltpu.VMEM((rows + 2 * HALO, cols), f32),
            pltpu.VMEM((local, rows + 2 * HALO, cols), f32),
            pltpu.VMEM(padded, f32),
            pltpu.VMEM(padded, f32),
            dma((2, chunks)),
            dma,
            dma((tm_size - 1, out_levels)),
            dma((tm_size - 1, out_levels)),
            dma((member_size - 1, out_levels)),
            dma((member_size - 1, out_levels)),
            dma((member_size - 1, out_levels)),
            dma((member_size - 1, out_levels)),
            dma((2, out_levels)),
            dma((2, out_levels)),
            dma((2,)),
            dma((2,)),
            dma((out_levels,)),
        ]
        hbm = pl.BlockSpec(memory_space=pl.ANY)
        return pl.pallas_call(
            functools.partial(kernel, tm_size, member_size, state_size, scale),
            out_shape=jax.ShapeDtypeStruct(block, f32),
            in_specs=[hbm, hbm, hbm, pl.BlockSpec(memory_space=pltpu.SMEM)],
            out_specs=hbm,
            scratch_shapes=scratch,
            compiler_params=pltpu.CompilerParams(
                collective_id=0, has_side_effects=True, vmem_limit_bytes=VMEM_BYTES
            ),
        )(members, slot_grad, diffusivity, vertical)

    in_specs = (
        P("tm", "member", None, "state", None),
        P("tm", None, "state", None),
        P("state", None),
        P(),
    )
    out_specs = P("tm", "member", "state", None)
    return jax.shard_map(body, mesh=mesh, in_specs=in_specs, out_specs=out_specs, check_vma=False)
```

```python
import functools

import jax
import jax.numpy as jnp
from jax import lax
from jax.experimental import pallas as pl
from jax.experimental.pallas import tpu as pltpu
from jax.sharding import PartitionSpec as P

NSTEP = 4
HALO = 8
CHUNK = 16
VMEM_BYTES = 64 * 1000 * 1000


def kernel(
    tm_size, member_size, state_size, scale,
    members_ref, grad_ref, diff_ref, vertical_ref, out_ref,
    mem_v, grad_v, part, send, recv, gauge, field, local_sum, total, rs_buf, edges,
    diff_v, fbuf, va, vb,
    in_sem, diff_sem, xs_sem, xr_sem, gs_sem, gr_sem, rss_sem, rsr_sem, ags_sem, agr_sem,
    hs_sem, hr_sem, ds_sem, dr_sem, out_sem,
):
    slots, local, levels, rows, cols = mem_v.shape
    out_levels = field.shape[0]
    ensemble = local * member_size
    width = cols // member_size
    tm = lax.axis_index("tm")
    mine = lax.axis_index("member")
    state = lax.axis_index("state")
    has_up, has_down = state > 0, state < state_size - 1
    chunks = rows // CHUNK

    def in_copies(c):
        at = pl.ds(c * CHUNK, CHUNK)
        return (
            pltpu.make_async_copy(
                members_ref.at[:, :, :, at, :], mem_v.at[:, :, :, at, :], in_sem.at[0, c]
            ),
            pltpu.make_async_copy(grad_ref.at[:, :, at, :], grad_v.at[:, :, at, :], in_sem.at[1, c]),
        )

    for c in range(chunks):
        for copy in in_copies(c):
            copy.start()
    diff_in = pltpu.make_async_copy(diff_ref, diff_v.at[pl.ds(HALO, rows), :], diff_sem)
    diff_in.start()

    barrier = pltpu.get_barrier_semaphore()
    for d in range(1, tm_size):
        pl.semaphore_signal(barrier, inc=1, device_id={"tm": lax.rem(tm + d, tm_size)})
    for d in range(1, member_size):
        pl.semaphore_signal(barrier, inc=1, device_id={"member": lax.rem(mine + d, member_size)})

    @pl.when(has_up)
    def _():
        pl.semaphore_signal(barrier, inc=1, device_id={"state": state - 1})

    @pl.when(has_down)
    def _():
        pl.semaphore_signal(barrier, inc=1, device_id={"state": state + 1})

    sides = has_up.astype(jnp.int32) + has_down.astype(jnp.int32)
    pl.semaphore_wait(barrier, tm_size + member_size - 2 + sides)

    slots_x = local * member_size

    def x_copy(d, lev, first, at):
        which = pl.ds(first, slots_x - first)
        return pltpu.make_async_remote_copy(
            src_ref=send.at[d - 1, lev, which, at, :],
            dst_ref=recv.at[d - 1, lev, which, at, :],
            send_sem=xs_sem.at[d - 1, lev],
            recv_sem=xr_sem.at[d - 1, lev],
            device_id={"tm": lax.rem(tm + d, tm_size)},
        )

    def gauge_copy(d, e, lev):
        return pltpu.make_async_remote_copy(
            src_ref=send.at[d - 1, lev, 0],
            dst_ref=gauge.at[d - 1, lev, e - 1],
            send_sem=gs_sem.at[d - 1, e - 1, lev],
            recv_sem=gr_sem.at[d - 1, e - 1, lev],
            device_id={"member": lax.rem(mine + e, member_size)},
        )

    def mix(source_level, store, tile0, tiles):
        def one(i, carry):
            m = lax.rem(i, local)
            at = pl.ds(pl.multiple_of((tile0 + i // local) * 8, 8), 8)
            acc = vertical_ref[0, source_level] * part[0, m, at, :]
            for j in range(1, levels):
                acc = acc + vertical_ref[j, source_level] * part[j, m, at, :]
            store(m, at, acc)
            return carry

        lax.fori_loop(0, tiles * local, one, 0)

    def places_before(owner):
        return lax.rem(mine + member_size - owner, member_size)

    def mix_send(d, lev, tile0, tiles):
        def store(m, at, acc):
            for owner in range(member_size):
                slot = m * member_size + places_before(owner)
                send[d - 1, lev, slot, at, :] = acc[:, owner * width : (owner + 1) * width]

        mix(send_level(d, lev), store, tile0, tiles)

    def mix_own(lev):
        def store(m, at, acc):
            field[lev, m, at, :] = acc

        mix(tm * out_levels + lev, store, 0, rows // 8)

    def send_level(d, lev):
        return lax.rem(tm + d, tm_size) * out_levels + lev

    for c in range(chunks):
        at = pl.ds(c * CHUNK, CHUNK)
        for copy in in_copies(c):
            copy.wait()

        def slot_sum(j, carry):
            for m in range(local):
                acc = mem_v[0, m, j, at, :].astype(jnp.float32) * grad_v[0, j, at, :]
                for s in range(1, slots):
                    acc = acc + mem_v[s, m, j, at, :].astype(jnp.float32) * grad_v[s, j, at, :]
                part[j, m, at, :] = acc
            return carry

        lax.fori_loop(0, levels, slot_sum, 0)
        for d in range(1, tm_size):
            mix_send(d, 0, c * (CHUNK // 8), CHUNK // 8)
            x_copy(d, 0, 0, at).start()

    full = pl.ds(0, rows)

    def open_level(lev):
        for d in range(1, tm_size):
            mix_send(d, lev, 0, rows // 8)
            for e in range(1, member_size):
                gauge_copy(d, e, lev).start()
            recv[d - 1, lev, 0] = jnp.zeros((rows, width), jnp.float32)

    def send_rest(lev):
        for d in range(1, tm_size):
            for e in range(1, member_size):
                gauge_copy(d, e, lev).wait_recv()

            def one(i, carry):
                at = pl.ds(pl.multiple_of(i * 8, 8), 8)
                for e in range(member_size):
                    common = send[d - 1, lev, 0, at, :] if e == 0 else gauge[d - 1, lev, e - 1, at, :]
                    for m in range(1 if e == 0 else 0, local):
                        slot = m * member_size + e
                        send[d - 1, lev, slot, at, :] = send[d - 1, lev, slot, at, :] - common
                return carry

            lax.fori_loop(0, rows // 8, one, 0)
            x_copy(d, lev, 1, full).start()

    def ahead(lev, carry):
        open_level(lev)
        mix_own(lev)
        send_rest(lev - 1)
        return carry

    open_level(1)
    mix_own(0)
    mix_own(1)
    lax.fori_loop(2, out_levels, ahead, 0)
    send_rest(out_levels - 1)

    diff_in.wait()

    def neighbour_copy(up, src, dst, send_sem, recv_sem):
        return pltpu.make_async_remote_copy(
            src_ref=src,
            dst_ref=dst,
            send_sem=send_sem,
            recv_sem=recv_sem,
            device_id={"state": state - 1 if up else state + 1},
        )

    def diff_copy(up):
        src = HALO if up else rows
        dst = rows + HALO if up else 0
        k = 1 if up else 0
        return neighbour_copy(
            up, diff_v.at[pl.ds(src, HALO), :], diff_v.at[pl.ds(dst, HALO), :], ds_sem.at[k], dr_sem.at[k]
        )

    def edge_copy(up, lev):
        src = 0 if up else rows - HALO
        k = 1 if up else 0
        return neighbour_copy(
            up, field.at[lev, :, pl.ds(src, HALO), :], edges.at[lev, k], hs_sem.at[k, lev], hr_sem.at[k, lev]
        )

    @pl.when(has_up)
    def _():
        diff_copy(True).start()

    @pl.when(has_down)
    def _():
        diff_copy(False).start()

    def clear_edges(k):
        diff_v[pl.ds(k * (rows + HALO), HALO), :] = jnp.zeros((HALO, cols), jnp.float32)

        def one(lev, carry):
            edges[lev, k] = jnp.zeros(edges.shape[2:], jnp.float32)
            return carry

        lax.fori_loop(0, out_levels, one, 0)

    @pl.when(jnp.logical_not(has_up))
    def _():
        clear_edges(0)

    @pl.when(jnp.logical_not(has_down))
    def _():
        clear_edges(1)

    for v in (va, vb):
        for m in range(local):
            v[m, pl.ds(0, 8), :] = jnp.zeros((8, cols), jnp.float32)
            v[m, pl.ds(rows + 2 * HALO + 8, 8), :] = jnp.zeros((8, cols), jnp.float32)

    @pl.when(has_up)
    def _():
        diff_copy(True).wait_send()
        diff_copy(False).wait_recv()

    @pl.when(has_down)
    def _():
        diff_copy(False).wait_send()
        diff_copy(True).wait_recv()

    def lane_slice(owner):
        return pl.ds(pl.multiple_of(owner * width, 128), width)

    def rs_copy(d, lev):
        peer = lax.rem(mine + d, member_size)
        return pltpu.make_async_remote_copy(
            src_ref=local_sum.at[lev, :, lane_slice(peer)],
            dst_ref=rs_buf.at[lev, d - 1],
            send_sem=rss_sem.at[d - 1, lev],
            recv_sem=rsr_sem.at[d - 1, lev],
            device_id={"member": peer},
        )

    def ag_copy(d, lev, owner):
        return pltpu.make_async_remote_copy(
            src_ref=total.at[lev, :, lane_slice(owner)],
            dst_ref=total.at[lev, :, lane_slice(owner)],
            send_sem=ags_sem.at[d - 1, lev],
            recv_sem=agr_sem.at[d - 1, lev],
            device_id={"member": lax.rem(mine + d, member_size)},
        )

    def arrive(lev, first):
        for d in range(1, tm_size):
            x_copy(d, lev, first, full).wait_recv()

        def one(i, carry):
            at = pl.ds(pl.multiple_of(i * 8, 8), 8)
            for owner in range(member_size):
                lanes = pl.ds(owner * width, width)
                acc = None
                for m in range(local):
                    value = field[lev, m, at, lanes]
                    for d in range(1, tm_size):
                        value = value + recv[d - 1, lev, m * member_size + places_before(owner), at, :]
                    field[lev, m, at, lanes] = value
                    acc = value if acc is None else acc + value
                local_sum[lev, at, lanes] = acc
            return carry

        lax.fori_loop(0, rows // 8, one, 0)
        for d in range(1, member_size):
            rs_copy(d, lev).start()

    def reduce(lev):
        for d in range(1, member_size):
            rs_copy(d, lev).wait_recv()
        at = lane_slice(mine)
        acc = local_sum[lev, :, at]
        for d in range(1, member_size):
            acc = acc + rs_buf[lev, d - 1]
        total[lev, :, at] = acc * (1.0 / ensemble)
        for d in range(1, member_size):
            ag_copy(d, lev, mine).start()

    def centre(lev):
        for d in range(1, member_size):
            ag_copy(d, lev, lax.rem(mine + member_size - d, member_size)).wait_recv()

        def one(i, carry):
            at = pl.ds(pl.multiple_of(i * 8, 8), 8)
            mean = total[lev, at, :]
            for m in range(local):
                field[lev, m, at, :] = (field[lev, m, at, :] - mean) * scale
            return carry

        lax.fori_loop(0, rows // 8, one, 0)

        @pl.when(has_up)
        def _():
            edge_copy(True, lev).start()

        @pl.when(has_down)
        def _():
            edge_copy(False, lev).start()

    tiles = (rows + 2 * HALO) // 8

    def filter_level(lev):
        @pl.when(has_up)
        def _():
            edge_copy(True, lev).wait_send()
            edge_copy(False, lev).wait_recv()

        @pl.when(has_down)
        def _():
            edge_copy(False, lev).wait_send()
            edge_copy(True, lev).wait_recv()

        def one(m, carry):
            for i in range(tiles):
                if i == 0:
                    value = edges[lev, 0, m]
                elif i == tiles - 1:
                    value = edges[lev, 1, m]
                else:
                    value = field[lev, m, pl.ds(8 * (i - 1), 8), :]
                fbuf[m, pl.ds(8 * i, 8), :] = value
                va[m, pl.ds(8 * i + 8, 8), :] = value * diff_v[pl.ds(8 * i, 8), :]
            now, later = va, vb
            for step in range(NSTEP):
                last = step == NSTEP - 1
                for i in range(1 if last else 0, tiles - 1 if last else tiles):
                    mid = now[m, pl.ds(8 * i + 8, 8), :]
                    value = (
                        fbuf[m, pl.ds(8 * i, 8), :]
                        + now[m, pl.ds(8 * i + 9, 8), :]
                        + now[m, pl.ds(8 * i + 7, 8), :]
                        + pltpu.roll(mid, 1, 1)
                        + pltpu.roll(mid, cols - 1, 1)
                        - 4.0 * mid
                    )
                    if last:
                        field[lev, m, pl.ds(8 * (i - 1), 8), :] = value
                    else:
                        fbuf[m, pl.ds(8 * i, 8), :] = value
                        later[m, pl.ds(8 * i + 8, 8), :] = value * diff_v[pl.ds(8 * i, 8), :]
                now, later = later, now
            return carry

        lax.fori_loop(0, local, one, 0)
        out_copy(lev).start()

    def out_copy(lev):
        return pltpu.make_async_copy(field.at[lev], out_ref.at[lev], out_sem.at[lev])

    arrive(0, 0)
    reduce(0)

    def step(lev, carry):
        arrive(lev, 1)
        centre(lev - 1)
        reduce(lev)
        filter_level(lev - 1)
        return carry

    lax.fori_loop(1, out_levels, step, 0)
    centre(out_levels - 1)
    filter_level(out_levels - 1)

    def finish(lev, first):
        for d in range(1, tm_size):
            x_copy(d, lev, first, full).wait_send()
            for e in range(1, member_size if first else 1):
                gauge_copy(d, e, lev).wait_send()
        for d in range(1, member_size):
            rs_copy(d, lev).wait_send()
            ag_copy(d, lev, mine).wait_send()
        out_copy(lev).wait()

    def finish_rest(lev, carry):
        finish(lev, 1)
        return carry

    finish(0, 0)
    lax.fori_loop(1, out_levels, finish_rest, 0)


def solution(mesh):
    tm_size, member_size, state_size = (mesh.shape[a] for a in ("tm", "member", "state"))

    def body(members, slot_grad, diffusivity, vertical):
        slots, local, levels, rows, cols = members.shape
        out_levels = levels // tm_size
        width = cols // member_size
        f32 = jnp.float32
        dma = pltpu.SemaphoreType.DMA
        chunks = rows // CHUNK
        scale = float(local * member_size - 1) ** -0.5
        block = (out_levels, local, rows, cols)
        padded = (local, rows + 2 * HALO + 16, cols)
        scratch = [
            pltpu.VMEM(members.shape, members.dtype),
            pltpu.VMEM(slot_grad.shape, f32),
            pltpu.VMEM((levels, local, rows, cols), f32),
            pltpu.VMEM((tm_size - 1, out_levels, local * member_size, rows, width), f32),
            pltpu.VMEM((tm_size - 1, out_levels, local * member_size, rows, width), f32),
            pltpu.VMEM((tm_size - 1, out_levels, member_size - 1, rows, width), f32),
            pltpu.VMEM(block, f32),
            pltpu.VMEM((out_levels, rows, cols), f32),
            pltpu.VMEM((out_levels, rows, cols), f32),
            pltpu.VMEM((out_levels, member_size - 1, rows, width), f32),
            pltpu.VMEM((out_levels, 2, local, HALO, cols), f32),
            pltpu.VMEM((rows + 2 * HALO, cols), f32),
            pltpu.VMEM((local, rows + 2 * HALO, cols), f32),
            pltpu.VMEM(padded, f32),
            pltpu.VMEM(padded, f32),
            dma((2, chunks)),
            dma,
            dma((tm_size - 1, out_levels)),
            dma((tm_size - 1, out_levels)),
            dma((tm_size - 1, member_size - 1, out_levels)),
            dma((tm_size - 1, member_size - 1, out_levels)),
            dma((member_size - 1, out_levels)),
            dma((member_size - 1, out_levels)),
            dma((member_size - 1, out_levels)),
            dma((member_size - 1, out_levels)),
            dma((2, out_levels)),
            dma((2, out_levels)),
            dma((2,)),
            dma((2,)),
            dma((out_levels,)),
        ]
        hbm = pl.BlockSpec(memory_space=pl.ANY)
        return pl.pallas_call(
            functools.partial(kernel, tm_size, member_size, state_size, scale),
            out_shape=jax.ShapeDtypeStruct(block, f32),
            in_specs=[hbm, hbm, hbm, pl.BlockSpec(memory_space=pltpu.SMEM)],
            out_specs=hbm,
            scratch_shapes=scratch,
            compiler_params=pltpu.CompilerParams(
                collective_id=0, has_side_effects=True, vmem_limit_bytes=VMEM_BYTES
            ),
        )(members, slot_grad, diffusivity, vertical)

    in_specs = (
        P("tm", "member", None, "state", None),
        P("tm", None, "state", None),
        P("state", None),
        P(),
    )
    out_specs = P("tm", "member", "state", None)
    return jax.shard_map(body, mesh=mesh, in_specs=in_specs, out_specs=out_specs, check_vma=False)
```
